32 devices in a mesh: dp: 32 (over z, y, x, core).
Axes of the slice: x: 2, y: 2, z: 4, core: 2. Of those that a mesh axis runs over, the one named last changes fastest.
Arguments:
- grad_qkv: bfloat16 [64, 768, 2304], P('dp')
- grad_o: bfloat16 [64, 768, 768], P('dp')
- grad_up: bfloat16 [64, 768, 3072], P('dp')
- grad_down: bfloat16 [64, 3072, 768], P('dp')
- w_qkv: float32 [2, 768, 2304], replicated
- w_o: float32 [2, 768, 768], replicated
- w_up: float32 [2, 768, 3072], replicated
- w_down: float32 [2, 3072, 768], replicated
- stat_left: float32 [7, 32, 256, 256], P(None, 'dp')
- stat_right: float32 [7, 32, 256, 256], P(None, 'dp')
- graft_var: float32 [7, 32, 256, 256], P(None, 'dp')
Outputs:
- output 1: float32 [2, 768, 2304], replicated
- output 2: float32 [2, 768, 768], replicated
- output 3: float32 [2, 768, 3072], replicated
- output 4: float32 [2, 3072, 768], replicated
- output 5: float32 [7, 32, 256, 256], P(None, 'dp')
- output 6: float32 [7, 32, 256, 256], P(None, 'dp')
- output 7: float32 [7, 32, 256, 256], P(None, 'dp')
All inputs are finite; a program needn't handle non-finite values.
Results may differ from the reference program's by a relative error of at most 0.001.
Values sent between devices are 32-bit elements.
A program may use at most 1 GiB of HBM per device.

```python
import jax
import jax.numpy as jnp
from jax import lax

LAYERS = 2
D = 768
QKV = 2304
FF = 3072
BLOCK = 256
DP_SIZE = 32
NEWTON_ITERS = 15
STEP_COUNT = 100

STAT_BETA = 0.999
EPS_ROOT = 1e-6
EPS_GRAFT = 1e-8
LR_RATE = 1e-3
WEIGHT_DECAY = 0.01
BIAS_FIX = 1.0 - STAT_BETA ** STEP_COUNT
VAR_LEVEL = 1.0 - STAT_BETA ** (STEP_COUNT - 1)
MAT_SHAPES = ((D, QKV), (D, D), (D, FF), (FF, D))
BLOCKS_LAYER = (D // BLOCK) * (QKV // BLOCK) + (D // BLOCK) * (D // BLOCK) + 2 * (D // BLOCK) * (FF // BLOCK)
BLOCKS_ALL = LAYERS * BLOCKS_LAYER
SLOT_COUNT = (BLOCKS_ALL + DP_SIZE - 1) // DP_SIZE
SLOTS_FLAT = SLOT_COUNT * DP_SIZE


def matmul(left_op, right_op):
    return jnp.dot(left_op, right_op, precision=lax.Precision.HIGHEST, preferred_element_type=jnp.float32)


def spd_draw(key):
    noise = jax.random.normal(key, (SLOTS_FLAT, BLOCK, 2 * BLOCK), jnp.float32)
    gram = jnp.einsum('sik,sjk->sij', noise, noise)
    return (gram * 0.0005).reshape(SLOT_COUNT, DP_SIZE, BLOCK, BLOCK)


def setup_inputs(seed: int = 0) -> dict:
    keys = jax.random.split(jax.random.key(seed), 11)
    grad_scale = DP_SIZE ** 0.5

    def grad_draw(key, n_rows, n_cols):
        def one_rank(rank_idx):
            values = jax.random.normal(jax.random.fold_in(key, rank_idx), (LAYERS, n_rows, n_cols), jnp.float32)
            return (values * grad_scale).astype(jnp.bfloat16)
        return lax.map(one_rank, jnp.arange(DP_SIZE)).reshape(DP_SIZE * LAYERS, n_rows, n_cols)

    def weight_draw(key, n_rows, n_cols):
        return jax.random.normal(key, (LAYERS, n_rows, n_cols), jnp.float32) * LR_RATE

    var_noise = jax.random.normal(keys[10], (SLOT_COUNT, DP_SIZE, BLOCK, BLOCK), jnp.float32)
    return {
        'grad_qkv': grad_draw(keys[0], D, QKV),
        'grad_o': grad_draw(keys[1], D, D),
        'grad_up': grad_draw(keys[2], D, FF),
        'grad_down': grad_draw(keys[3], FF, D),
        'w_qkv': weight_draw(keys[4], D, QKV),
        'w_o': weight_draw(keys[5], D, D),
        'w_up': weight_draw(keys[6], D, FF),
        'w_down': weight_draw(keys[7], FF, D),
        'stat_left': spd_draw(keys[8]),
        'stat_right': spd_draw(keys[9]),
        'graft_var': VAR_LEVEL * (0.25 + var_noise * var_noise),
    }


def inverse_root(stat_mat):
    identity = jnp.eye(BLOCK, dtype=jnp.float32)
    shifted = stat_mat + EPS_ROOT * identity
    frob_norm = jnp.sqrt(jnp.sum(shifted * shifted))

    def newton_step(newton_state, unused):
        root_x, mat_m = newton_state
        factor = (5.0 * identity - mat_m) / 4.0
        factor_sq = matmul(factor, factor)
        return (matmul(root_x, factor), matmul(matmul(factor_sq, factor_sq), mat_m)), None

    newton_state, unused = lax.scan(newton_step, (identity * frob_norm ** -0.25, shifted / frob_norm), None, length=NEWTON_ITERS)
    return newton_state[0]


def block_step(operands):
    grad_block, left_stat, right_stat, var_stat = operands
    left_new = STAT_BETA * left_stat + (1.0 - STAT_BETA) * matmul(grad_block, grad_block.T)
    right_new = STAT_BETA * right_stat + (1.0 - STAT_BETA) * matmul(grad_block.T, grad_block)
    var_new = STAT_BETA * var_stat + (1.0 - STAT_BETA) * grad_block * grad_block
    precond = matmul(matmul(inverse_root(left_new), grad_block), inverse_root(right_new))
    adam_dir = grad_block / (jnp.sqrt(var_new / BIAS_FIX) + EPS_GRAFT)
    direction = precond * (jnp.sqrt(jnp.sum(adam_dir * adam_dir)) / jnp.sqrt(jnp.sum(precond * precond)))
    return direction, left_new, right_new, var_new


def to_blocks(matrices):
    pieces = []
    for matrix in matrices:
        n_rows, n_cols = matrix.shape[1], matrix.shape[2]
        tiled = matrix.reshape(LAYERS, n_rows // BLOCK, BLOCK, n_cols // BLOCK, BLOCK).transpose(0, 1, 3, 2, 4)
        pieces.append(tiled.reshape(LAYERS, -1, BLOCK, BLOCK))
    return jnp.concatenate(pieces, axis=1).reshape(BLOCKS_ALL, BLOCK, BLOCK)


def from_blocks(blocks):
    per_layer = blocks.reshape(LAYERS, BLOCKS_LAYER, BLOCK, BLOCK)
    matrices = []
    offset = 0
    for n_rows, n_cols in MAT_SHAPES:
        tile_count = (n_rows // BLOCK) * (n_cols // BLOCK)
        tiled = per_layer[:, offset:offset + tile_count].reshape(LAYERS, n_rows // BLOCK, n_cols // BLOCK, BLOCK, BLOCK)
        matrices.append(tiled.transpose(0, 1, 3, 2, 4).reshape(LAYERS, n_rows, n_cols))
        offset = offset + tile_count
    return matrices


def reference(grad_qkv, grad_o, grad_up, grad_down, w_qkv, w_o, w_up, w_down, stat_left, stat_right, graft_var):
    mean_grads = [jnp.sum(grad_stack.reshape(DP_SIZE, LAYERS, grad_stack.shape[1], grad_stack.shape[2]), axis=0, dtype=jnp.float32) / DP_SIZE for grad_stack in (grad_qkv, grad_o, grad_up, grad_down)]
    blocks = to_blocks(mean_grads)
    flat_left = stat_left.reshape(SLOTS_FLAT, BLOCK, BLOCK)
    flat_right = stat_right.reshape(SLOTS_FLAT, BLOCK, BLOCK)
    flat_var = graft_var.reshape(SLOTS_FLAT, BLOCK, BLOCK)
    directions, left_new, right_new, var_new = lax.map(block_step, (blocks, flat_left[:BLOCKS_ALL], flat_right[:BLOCKS_ALL], flat_var[:BLOCKS_ALL]))
    step_dirs = from_blocks(directions)
    new_weights = [weight - LR_RATE * (step_dir + WEIGHT_DECAY * weight) for weight, step_dir in zip((w_qkv, w_o, w_up, w_down), step_dirs)]

    def restore(new_part, old_flat):
        return jnp.concatenate([new_part, old_flat[BLOCKS_ALL:]], axis=0).reshape(SLOT_COUNT, DP_SIZE, BLOCK, BLOCK)

    return (new_weights[0], new_weights[1], new_weights[2], new_weights[3], restore(left_new, flat_left), restore(right_new, flat_right), restore(var_new, flat_var))
```

```python
import functools

import jax
import jax.numpy as jnp
from jax import lax
from jax.experimental import pallas as pl
from jax.experimental.pallas import tpu as pltpu
from jax.sharding import PartitionSpec as P

STAT_BETA = 0.999
EPS_ROOT = 1e-6
EPS_GRAFT = 1e-8
LR_RATE = 1e-3
WEIGHT_DECAY = 0.01
NEWTON_ITERS = 15
STEP_COUNT = 100
BIAS_FIX = 1.0 - STAT_BETA ** STEP_COUNT

RANKS = 32
HALVES = 2
MESH = pl.DeviceIdType.MESH
F32 = jnp.float32


def flipped(bit, flip):
    return bit + flip - 2 * bit * flip


def place():
    me = lax.axis_index('dp')
    core = me % 2
    x, y, za, zb = (me // 2) % 2, (me // 4) % 2, (me // 8) % 2, me // 16
    stride1, bit1 = 2 + 2 * core, x + core * (y - x)
    stride3, bit3 = 4 - 2 * core, y + core * (x - y)
    partners = (
        me + 1 - 2 * core,
        me + stride1 * (1 - 2 * bit1),
        me + 8 * (1 - 2 * za),
        me + stride3 * (1 - 2 * bit3),
        me + 16 * (1 - 2 * zb),
    )
    return me, (core, x, y, za, zb), partners


def owner_at(coords, pos, core):
    _, x, y, za, zb = coords
    b1, b2, b3, b4 = (pos // 8) % 2, (pos // 4) % 2, (pos // 2) % 2, pos % 2
    fx, fy = b1 + core * (b3 - b1), b3 + core * (b1 - b3)
    return flipped(zb, b4) * 16 + flipped(za, b2) * 8 + flipped(y, fy) * 4 + flipped(x, fx) * 2 + core


class Tiling:
    def __init__(self, shapes, block):
        self.block = block
        self.layers = shapes[0][0]
        self.spans = []
        start = 0
        for _, rows, cols in shapes:
            count = (rows // block) * (cols // block)
            self.spans.append((start, start + count, cols // block))
            start += count
        self.per_layer = start
        self.total = start * self.layers

    def visit(self, number, half, fn):
        layer, local = number // self.per_layer, number % self.per_layer
        rows = self.block // HALVES
        for index, (low, high, width) in enumerate(self.spans):
            @pl.when((local >= low) & (local < high))
            def _():
                row, col = (local - low) // width, (local - low) % width
                fn(index, layer, pl.ds(pl.multiple_of(row * self.block + half * rows, rows), rows),
                   pl.ds(pl.multiple_of(col * self.block, self.block), self.block))


def enter(partners):
    barrier = pltpu.get_barrier_semaphore()
    for partner in partners:
        pl.semaphore_signal(barrier, inc=1, device_id=(partner,), device_id_type=MESH)
    pl.semaphore_wait(barrier, len(partners))


def split(value):
    high = value.astype(jnp.bfloat16)
    rest = value - high.astype(F32)
    mid = rest.astype(jnp.bfloat16)
    return high, mid, (rest - mid.astype(F32)).astype(jnp.bfloat16)


def pieces(left, right):
    return jnp.dot(left, right, preferred_element_type=F32)


def product(left, right):
    a1, a2, a3 = left
    b1, b2, b3 = right
    return (pieces(a3, b1) + pieces(a2, b2) + pieces(a1, b3) + pieces(a2, b1) + pieces(a1, b2)) + pieces(a1, b1)


def total(value):
    return jnp.sum(jnp.sum(value, axis=0, keepdims=True), axis=1, keepdims=True)


TICKS = 15
HALF_STEP = 8
OFFSETS = {'load': 0, 'e0': 2, 'e1': 5, 'e2': 15, 'e3': 25, 'e4': 30, 'e5': 35}
LATENCY = 3
N_SEND, N_A, N_B, N_ACC, N_RECV = 2, 2, 3, 6, 4


def reduce_kernel(tiling, slots, g_qkv, g_o, g_up, g_down, l_in, r_in, v_in, l_out, r_out, v_out, u_out,
                  a_buf, b_buf, send0, acc, recv1, recv2, recv3, recv4, grad, stats, staged, u_buf, xs, ms, norms,
                  load_sem, send_sem, recv_sem, stat_sem, out_sem, u_sem):
    me, coords, partners = place()
    core = coords[0]
    block = tiling.block
    rows = block // HALVES
    units = slots * HALVES
    grads = (g_qkv, g_o, g_up, g_down)
    recvs = (None, recv1, recv2, recv3, recv4)

    def loads(unit, which):
        return pltpu.make_async_copy((a_buf, b_buf)[which].at[unit % (N_A, N_B)[which]],
                                     (a_buf, b_buf)[which].at[unit % (N_A, N_B)[which]],
                                     load_sem.at[which, unit % (N_A, N_B)[which]])

    def remote(stage, unit):
        slot = unit % N_ACC
        if stage == 0:
            src, dst = send0.at[unit % N_SEND], acc.at[slot]
        else:
            size = 16 >> stage
            src, dst = acc.at[slot, pl.ds(size, size)], recvs[stage].at[unit % N_RECV]
        return pltpu.make_async_remote_copy(src, dst, send_sem.at[stage, slot], recv_sem.at[stage, slot],
                                            device_id=(partners[stage],), device_id_type=MESH)

    def load(unit):
        slot, half = unit // HALVES, unit % HALVES

        def one(pos, _):
            for which, owner_core in ((0, 1 - core), (1, core)):
                number = slot * RANKS + owner_at(coords, pos, owner_core)
                number = number - RANKS * (number // tiling.total)
                buf, n = ((a_buf, N_A), (b_buf, N_B))[which]

                def start(index, layer, rws, cls):
                    pltpu.make_async_copy(grads[index].at[layer, rws, cls], buf.at[unit % n, pos],
                                          load_sem.at[which, unit % n]).start()
                tiling.visit(number, half, start)
            return 0
        lax.fori_loop(0, 16, one, 0)

    def e0(unit):
        loads(unit, 0).wait()

        def one(pos, _):
            send0[unit % N_SEND, pos] = a_buf[unit % N_A, pos].astype(F32)
            return 0
        lax.fori_loop(0, 16, one, 0)
        remote(0, unit).start()

    def e1(unit):
        loads(unit, 1).wait()
        remote(0, unit).wait()

        def one(back, _):
            pos = 15 - back
            acc[unit % N_ACC, pos] += b_buf[unit % N_B, pos].astype(F32)
            return 0
        lax.fori_loop(0, 16, one, 0)
        remote(1, unit).start()

    def step(stage, unit):
        remote(stage, unit).wait()
        size = 16 >> stage

        def one(back, _):
            pos = size - 1 - back
            acc[unit % N_ACC, pos] += recvs[stage][unit % N_RECV, pos]
            return 0
        lax.fori_loop(0, size, one, 0)
        remote(stage + 1, unit).start()

    def e5(unit):
        remote(4, unit).wait()
        half = unit % HALVES
        grad[(unit // HALVES) % 2, pl.ds(pl.multiple_of(half * rows, rows), rows), :] = (
            acc[unit % N_ACC, 0] + recv4[unit % N_RECV, 0]) * (1.0 / RANKS)

    events = {'load': load, 'e0': e0, 'e1': e1, 'e2': functools.partial(step, 1), 'e3': functools.partial(step, 2),
              'e4': functools.partial(step, 3), 'e5': e5}

    def stat_copies(slot):
        return [pltpu.make_async_copy(ref.at[slot], stats.at[i], stat_sem.at[i]) for i, ref in enumerate((l_in, r_in, v_in))]

    def out_copies(slot):
        return [pltpu.make_async_copy(staged.at[i], ref.at[slot], out_sem.at[i]) for i, ref in enumerate((l_out, r_out, v_out))]

    def u_copy(slot):
        return pltpu.make_async_copy(u_buf, u_out.at[slot], u_sem)

    row_id = lax.broadcasted_iota(jnp.int32, (block, block), 0)
    col_id = lax.broadcasted_iota(jnp.int32, (block, block), 1)

    def ident():
        return jnp.where(row_id == col_id, 1.0, 0.0).astype(F32)

    def factor(mat):
        return (5.0 * ident() - mat) * 0.25

    def power4(parts):
        square = split(product(parts, parts))
        return split(product(square, square))

    def before(slot):
        for copy in stat_copies(slot):
            copy.wait()
        valid = slot * RANKS + me < tiling.total
        g = grad[slot % 2]
        g_parts, gt_parts = split(g), split(g.T)
        var = stats[2]
        var_new = STAT_BETA * var + (1.0 - STAT_BETA) * g * g
        staged[2] = jnp.where(valid, var_new, var)
        adam = g / (jnp.sqrt(var_new / BIAS_FIX) + EPS_GRAFT)
        norms[...] = jnp.broadcast_to(jnp.sqrt(total(adam * adam)), norms.shape)
        for i, (left, right) in enumerate(((g_parts, gt_parts), (gt_parts, g_parts))):
            old = stats[i]
            new = STAT_BETA * old + (1.0 - STAT_BETA) * product(left, right)
            staged[i] = jnp.where(valid, new, old)
            shifted = new + EPS_ROOT * ident()
            frob = jnp.sqrt(total(shifted * shifted))
            mat = shifted / frob
            t = factor(mat)
            xs[i] = lax.rsqrt(jnp.sqrt(frob)) * t
            ms[i] = product(power4(split(t)), split(mat))

    def newton():
        ts = [split(factor(ms[i])) for i in range(2)]
        squares = [split(product(t, t)) for t in ts]
        for i in range(2):
            xs[i] = product(split(xs[i]), ts[i])
        fourths = [split(product(sq, sq)) for sq in squares]
        for i in range(2):
            ms[i] = product(fourths[i], split(ms[i]))

    def after(slot):
        roots = [split(product(split(xs[i]), split(factor(ms[i])))) for i in range(2)]
        g_parts = split(grad[slot % 2])
        precond = product(split(product(roots[0], g_parts)), roots[1])
        scale = norms[0:1, 0:1] / jnp.sqrt(total(precond * precond))
        u_buf[...] = precond * scale

    def compute(slot, tick):
        inside = (slot >= 0) & (slot < slots)

        @pl.when(inside & (tick == 0))
        def _():
            before(slot)

        @pl.when(inside & (tick > 0) & (tick < TICKS - 1))
        def _():
            newton()

        @pl.when(inside & (tick == TICKS - 1))
        def _():
            after(slot)

        @pl.when(inside & (tick == 1))
        def _():
            for copy in out_copies(slot):
                copy.start()

        @pl.when((slot >= -1) & (slot < slots - 1) & (tick == 2))
        def _():
            for copy in stat_copies(slot + 1):
                copy.start()

        @pl.when(inside & (tick == TICKS - 2))
        def _():
            for copy in out_copies(slot):
                copy.wait()

        @pl.when((slot >= 1) & (slot < slots) & (tick == 1))
        def _():
            u_copy(slot - 1).start()

        @pl.when((slot >= 1) & (slot < slots) & (tick == TICKS - 2))
        def _():
            u_copy(slot - 1).wait()

    enter(partners)

    def period(s, _):
        def one_tick(tick, _):
            for name in ('e5', 'e4', 'e3', 'e2', 'e1', 'e0', 'load'):
                for half in range(HALVES):
                    offset = OFFSETS[name] + HALF_STEP * half
                    slot = s - offset // TICKS

                    @pl.when((tick == offset % TICKS) & (slot >= 0) & (slot < slots))
                    def _(name=name, half=half, slot=slot):
                        events[name](slot * HALVES + half)
            compute(s - LATENCY, tick)
            return 0
        lax.fori_loop(0, TICKS, one_tick, 0)
        return 0
    lax.fori_loop(0, slots + LATENCY, period, 0)
    u_copy(slots - 1).start()
    u_copy(slots - 1).wait()


def reduce_and_direct(tiling, grads, stats, collective_id):
    slots, block = stats[0].shape[0], tiling.block
    rows = block // HALVES
    stat_shape = jax.ShapeDtypeStruct((slots, block, block), F32)
    hbm = pl.BlockSpec(memory_space=pl.ANY)
    dma = pltpu.SemaphoreType.DMA
    return pl.pallas_call(
        functools.partial(reduce_kernel, tiling, slots),
        out_shape=[stat_shape] * 4,
        in_specs=[hbm] * 7,
        out_specs=[hbm] * 4,
        scratch_shapes=[
            pltpu.VMEM((N_A, 16, rows, block), jnp.bfloat16),
            pltpu.VMEM((N_B, 16, rows, block), jnp.bfloat16),
            pltpu.VMEM((N_SEND, 16, rows, block), F32),
            pltpu.VMEM((N_ACC, 16, rows, block), F32),
            pltpu.VMEM((N_RECV, 8, rows, block), F32),
            pltpu.VMEM((N_RECV, 4, rows, block), F32),
            pltpu.VMEM((N_RECV, 2, rows, block), F32),
            pltpu.VMEM((N_RECV, 1, rows, block), F32),
            pltpu.VMEM((2, block, block), F32),
            pltpu.VMEM((3, block, block), F32),
            pltpu.VMEM((3, block, block), F32),
            pltpu.VMEM((block, block), F32),
            pltpu.VMEM((2, block, block), F32),
            pltpu.VMEM((2, block, block), F32),
            pltpu.VMEM((8, 128), F32),
            dma((2, max(N_A, N_B))),
            dma((5, N_ACC)),
            dma((5, N_ACC)),
            dma((3,)),
            dma((3,)),
            dma,
        ],
        compiler_params=pltpu.CompilerParams(collective_id=collective_id, has_side_effects=True,
                                             vmem_limit_bytes=60 * 1024 * 1024),
        name='reduce_and_direct',
    )(*grads, *stats)


N_GATH, N_W = 6, 3


def update_kernel(tiling, slots, u_in, w_qkv, w_o, w_up, w_down, n_qkv, n_o, n_up, n_down,
                  gath, w_buf, own_sem, send_sem, recv_sem, wload_sem, wstore_sem):
    me, coords, partners = place()
    core = coords[0]
    block = tiling.block
    rows = block // HALVES
    units = slots * HALVES
    weights = (w_qkv, w_o, w_up, w_down)
    results = (n_qkv, n_o, n_up, n_down)
    rest = tiling.total - (slots - 1) * RANKS

    def own(unit):
        half = unit % HALVES
        return pltpu.make_async_copy(u_in.at[unit // HALVES, pl.ds(pl.multiple_of(half * rows, rows), rows), :],
                                     gath.at[unit % N_GATH, 0], own_sem.at[unit % N_GATH])

    def remote(stage, unit):
        b = unit % N_GATH
        size = 16 >> stage
        return pltpu.make_async_remote_copy(gath.at[b, pl.ds(0, size)], gath.at[b, pl.ds(size, size)],
                                            send_sem.at[stage, b], recv_sem.at[stage, b],
                                            device_id=(partners[stage],), device_id_type=MESH)

    def each_tile(unit, fn):
        slot, half = unit // HALVES, unit % HALVES

        def one(pos, _):
            other = pos // 16
            owner = owner_at(coords, pos, core + other * (1 - 2 * core))
            number = slot * RANKS + owner

            @pl.when(number < tiling.total)
            def _():
                tiling.visit(number, half, lambda index, layer, rws, cls: fn(index, pos, layer, rws, cls))
            return 0
        lax.fori_loop(0, RANKS, one, 0)

    def w_load(unit):
        b = unit % N_W
        each_tile(unit, lambda index, pos, layer, rws, cls: pltpu.make_async_copy(
            weights[index].at[layer, rws, cls], w_buf.at[b, pos], wload_sem.at[b]).start())

    def w_store(unit):
        b = unit % N_W
        each_tile(unit, lambda index, pos, layer, rws, cls: pltpu.make_async_copy(
            w_buf.at[b, pos], results[index].at[layer, rws, cls], wstore_sem.at[b]).start())

    def w_wait(unit, sem):
        b = unit % N_W
        for count, cond in ((RANKS, unit // HALVES < slots - 1), (rest, unit // HALVES == slots - 1)):
            @pl.when(cond)
            def _():
                part = w_buf.at[b, pl.ds(0, count)]
                pltpu.make_async_copy(part, part, sem.at[b]).wait()

    def a1(unit):
        own(unit).wait()
        remote(4, unit).start()

    def step(stage, unit):
        remote(stage, unit).wait()
        remote(stage - 1, unit).start()

    def a6(unit):
        remote(0, unit).wait()
        w_wait(unit, wload_sem)

        def one(pos, _):
            w = w_buf[unit % N_W, pos]
            w_buf[unit % N_W, pos] = w - LR_RATE * (gath[unit % N_GATH, pos] + WEIGHT_DECAY * w)
            return 0
        lax.fori_loop(0, RANKS, one, 0)
        w_store(unit)

        @pl.when(unit > 0)
        def _():
            w_wait(unit - 1, wstore_sem)

        @pl.when(unit + 2 < units)
        def _():
            w_load(unit + 2)

    events = ((5, a6), (4, functools.partial(step, 1)), (3, functools.partial(step, 2)),
              (2, functools.partial(step, 3)), (1, functools.partial(step, 4)), (0, a1))

    enter(partners)
    own(0).start()
    w_load(0)
    w_load(1)

    def one_step(i, _):
        for lag, event in events:
            unit = i - lag

            @pl.when((unit >= 0) & (unit < units))
            def _(event=event, unit=unit):
                event(unit)

        @pl.when(i + 1 < units)
        def _():
            own(i + 1).start()
        return 0
    lax.fori_loop(0, units + 5, one_step, 0)
    w_wait(units - 1, wstore_sem)


def gather_and_update(tiling, direction, weights, collective_id):
    slots, block = direction.shape[0], tiling.block
    rows = block // HALVES
    hbm = pl.BlockSpec(memory_space=pl.ANY)
    dma = pltpu.SemaphoreType.DMA
    return pl.pallas_call(
        functools.partial(update_kernel, tiling, slots),
        out_shape=[jax.ShapeDtypeStruct(w.shape, F32) for w in weights],
        in_specs=[hbm] * 5,
        out_specs=[hbm] * 4,
        scratch_shapes=[
            pltpu.VMEM((N_GATH, RANKS, rows, block), F32),
            pltpu.VMEM((N_W, RANKS, rows, block), F32),
            dma((N_GATH,)),
            dma((5, N_GATH)),
            dma((5, N_GATH)),
            dma((N_W,)),
            dma((N_W,)),
        ],
        compiler_params=pltpu.CompilerParams(collective_id=collective_id, has_side_effects=True,
                                             vmem_limit_bytes=60 * 1024 * 1024),
        name='gather_and_update',
    )(direction, *weights)


def solution(mesh):
    assert mesh.shape['dp'] == RANKS

    def local_step(g_qkv, g_o, g_up, g_down, w_qkv, w_o, w_up, w_down, left_stat, right_stat, var_stat):
        weights = (w_qkv, w_o, w_up, w_down)
        slots, block = left_stat.shape[0], left_stat.shape[-1]
        tiling = Tiling([w.shape for w in weights], block)
        stats = [stat.reshape(slots, block, block) for stat in (left_stat, right_stat, var_stat)]
        left, right, var, direction = reduce_and_direct(tiling, (g_qkv, g_o, g_up, g_down), stats, 0)
        new_weights = gather_and_update(tiling, direction, weights, 1)
        return tuple(new_weights) + tuple(s.reshape(left_stat.shape) for s in (left, right, var))

    grad_spec = P('dp')
    stat_spec = P(None, 'dp')
    return jax.shard_map(local_step, mesh=mesh, in_specs=(grad_spec,) * 4 + (P(),) * 4 + (stat_spec,) * 3,
                         out_specs=(P(),) * 4 + (stat_spec,) * 3, check_vma=False)
```
